128 devices in a mesh: py: 4 (over x_lo, core), px: 32 (over z, y, x_hi).
Axes of the slice: x: 4 (x_hi: 2, x_lo: 2; x = x_hi * 2 + x_lo), y: 4, z: 4, core: 2. Of those that a mesh axis runs over, the one named last changes fastest.
Arguments:
- source_terms: float32 [256, 4096, 256], P('py', 'px'), may hold values from -6 to 6
- initial_values: float32 [256, 4096, 256], P('py', 'px'), may hold values from -6 to 6
- absorption: float32 [256, 4096, 256], P('py', 'px'), may hold values from 0.1 to 0.9
Outputs:
- solution: float32 [256, 4096, 256], P('py', 'px')
- remaining: float32 [256, 4096, 256], P('py', 'px')
The draws below stay inside these ranges and needn't reach their ends.
All inputs are finite; a program needn't handle non-finite values.
Results may differ from the reference program's by a relative error of at most 0.000033.
Values sent between devices are 32-bit elements; how exact they have to be, the bound alone decides.
A program may use at most 128 MiB of HBM per device.

```python
import jax
import jax.numpy as jnp
from jax import lax

LAYERS = 256
RATIO = 2
BEFORE = 2
AFTER = 2
INNER = 9
GRID_Y = 256
GRID_X = 4096


def shard_levels(stream_key, shape, split, smallest, top_value):
    def one(axis_at, blocks):
        steps = jax.random.uniform(jax.random.fold_in(jax.random.fold_in(stream_key, 6), axis_at), (blocks,), jnp.float32, smallest / len(split), top_value / len(split))
        return jnp.repeat(jnp.exp(steps), shape[axis_at] // blocks).reshape((-1,) + (1,) * (len(shape) - axis_at - 1))

    level = one(*split[0])
    for cut in split[1:]:
        level = level * one(*cut)
    return level


def gaussian(stream_key, extent, deviation, bound, shards=(), kind=jnp.bfloat16):
    array = jax.random.normal(stream_key, extent, jnp.float32) * deviation
    if len(shards) > 0:
        array = shard_levels(stream_key, extent, shards, -0.22, 0.18) * array
    return jnp.clip(array, min=-bound, max=bound).astype(kind)


def setup_inputs(seed: int = 0) -> dict:
    key_of = jax.random.split(jax.random.key(seed), 4)
    source_terms = gaussian(key_of[0], (GRID_Y, GRID_X, LAYERS), 1.0, 6.0, ((0, 4), (1, 32)), jnp.float32)
    initial_values = gaussian(key_of[1], (GRID_Y, GRID_X, LAYERS), 1.0, 6.0, ((0, 4), (1, 32)), jnp.float32)
    absorption = jnp.clip(0.1 + 0.79999997 * jax.random.uniform(key_of[2], (GRID_Y, GRID_X, LAYERS), jnp.float32) ** shard_levels(key_of[2], (GRID_Y, GRID_X, LAYERS), ((0, 4), (1, 32)), -0.2, 0.2), 0.1, 0.9)
    return dict(source_terms=source_terms, initial_values=initial_values, absorption=absorption)


def around_sum(padded):
    inner_y, inner_x = padded.shape[0] - 2, padded.shape[1] - 2
    middle_rows = lax.slice_in_dim(padded, 1, 1 + inner_y, axis=0)
    middle_columns = lax.slice_in_dim(padded, 1, 1 + inner_x, axis=1)
    return (lax.slice_in_dim(middle_columns, 0, inner_y, axis=0) + lax.slice_in_dim(middle_columns, 2, 2 + inner_y, axis=0)
            + lax.slice_in_dim(middle_rows, 0, inner_x, axis=1) + lax.slice_in_dim(middle_rows, 2, 2 + inner_x, axis=1))


def relax_once(padded, values, load, mass_here):
    return values + 0.8 * (load + around_sum(padded) - (4.0 + mass_here) * values) / (4.0 + mass_here)


def block_means(values):
    cut = values.reshape(values.shape[0] // RATIO, RATIO, values.shape[1] // RATIO, RATIO, values.shape[2])
    return jnp.mean(cut, axis=(1, 3))


def spread_blocks(values):
    return jnp.repeat(jnp.repeat(values, RATIO, axis=0), RATIO, axis=1)


def reference(source_terms, initial_values, absorption):
    values = initial_values
    for sweep in range(BEFORE):
        values = relax_once(jnp.pad(values, ((1, 1), (1, 1), (0, 0)), mode="wrap"), values, source_terms, absorption)
    defect = source_terms + around_sum(jnp.pad(values, ((1, 1), (1, 1), (0, 0)), mode="wrap")) - (4.0 + absorption) * values
    coarse_load, coarse_mass = block_means(defect) * RATIO, block_means(absorption) * RATIO
    coarse_values = jnp.zeros_like(coarse_load)
    for sweep in range(INNER):
        coarse_values = relax_once(jnp.pad(coarse_values, ((1, 1), (1, 1), (0, 0)), mode="wrap"), coarse_values, coarse_load, coarse_mass)
    values = values + spread_blocks(coarse_values)
    for sweep in range(AFTER):
        values = relax_once(jnp.pad(values, ((1, 1), (1, 1), (0, 0)), mode="wrap"), values, source_terms, absorption)
    solution = values
    remaining = source_terms + around_sum(jnp.pad(solution, ((1, 1), (1, 1), (0, 0)), mode="wrap")) - (4.0 + absorption) * solution
    return solution, remaining
```

```python
import functools

import jax
import jax.numpy as jnp
from jax import lax
from jax.experimental import pallas as pl
from jax.experimental.pallas import tpu as pltpu
from jax.sharding import PartitionSpec as P

MESH = pl.DeviceIdType.MESH
LANES = 128
FIRST = 4
SECOND = 5
OY, OX = 1, 8
CY, CX = SECOND, 8
SIDES = ((0, 1), (0, -1), (1, 0), (-1, 0))
AROUND = SIDES + ((1, 1), (1, -1), (-1, 1), (-1, -1))
U0, U1, U2, WEIGHT, LOAD, COARSE, U4, U5 = range(8)
UP, DOWN = 0, 1


def cut(direction, origin, size, depth, arriving):
    if direction == 0:
        return pl.ds(origin, size)
    if direction > 0:
        return pl.ds(origin - depth, depth) if arriving else pl.ds(origin + size - depth, depth)
    return pl.ds(origin + size, depth) if arriving else pl.ds(origin, depth)


def kernel(
    sizes, load_in, start_in, mass_in, sol, rem, u, f, wide_load, wide_weight, wide_values, swap, spread,
    local_sem, send_sem, recv_sem,
):
    ny, nx, chunks = sizes
    my, mx = ny // 2, nx // 2
    groups = nx // 8
    inner = tuple(range(1, groups - 1))
    rims = (0, groups - 1)
    every = tuple(range(groups))
    size_y, size_x = lax.axis_size("py"), lax.axis_size("px")
    at_y, at_x = lax.axis_index("py"), lax.axis_index("px")

    def device(dy, dx):
        return (lax.rem(at_y + dy + size_y, size_y), lax.rem(at_x + dx + size_x, size_x))

    def lanes(c):
        return pl.ds(c * LANES, LANES)

    fetched = []
    for c in range(chunks):
        for k, (src, dst) in enumerate((
            (mass_in, rem.at[:, :, lanes(c)]),
            (start_in, u.at[c, 0, pl.ds(OY, ny), pl.ds(OX, nx), :]),
            (load_in, f.at[c]),
        )):
            copy = pltpu.make_async_copy(src.at[:, :, lanes(c)], dst, local_sem.at[3 * c + k])
            copy.start()
            fetched.append(copy)

    barrier = pltpu.get_barrier_semaphore()
    for dy, dx in AROUND:
        pl.semaphore_signal(barrier, inc=1, device_id=device(dy, dx), device_id_type=MESH)
    pl.semaphore_wait(barrier, len(AROUND))

    flying = {}

    def send(c, tag, source, target, directions):
        copies = []
        for k, (dy, dx) in enumerate(directions):
            copy = pltpu.make_async_remote_copy(
                src_ref=source(dy, dx),
                dst_ref=target(dy, dx),
                send_sem=send_sem.at[c, tag, k],
                recv_sem=recv_sem.at[c, tag, k],
                device_id=device(dy, dx),
                device_id_type=MESH,
            )
            copy.start()
            copies.append(copy)
        flying[c, tag] = copies

    def arrive(c, tag):
        for copy in flying.pop((c, tag)):
            copy.wait()

    def fine_part(ref, dy, dx, arriving):
        return ref.at[cut(dy, OY, ny, 1, arriving), cut(dx, OX, nx, 1, arriving), :]

    def coarse_part(ref, dy, dx, depth, arriving):
        return ref.at[cut(dy, CY, my, depth, arriving), cut(dx, CX, mx, depth, arriving), :]

    def send_fine(c, tag, b):
        send(c, tag, lambda dy, dx: fine_part(u.at[c, b], dy, dx, False),
             lambda dy, dx: fine_part(u.at[c, b], dy, dx, True), SIDES)

    def send_coarse(c, tag, ref, depth):
        send(c, tag, lambda dy, dx: coarse_part(ref, dy, dx, depth, False),
             lambda dy, dx: coarse_part(ref, dy, dx, depth, True), AROUND)

    def start_edge(c, dy, dx):
        return start_in.at[cut(dy, 0, ny, 1, False), cut(dx, 0, nx, 1, False), lanes(c)]

    for c in range(chunks):
        send(c, U0, functools.partial(start_edge, c), lambda dy, dx: fine_part(u.at[c, 0], dy, dx, True), SIDES)

    def over(first, rows, count, body):
        def step(i, carry):
            body(first + i * rows)
            return carry
        lax.fori_loop(0, count, step, 0)

    def stencil(c, b, y, rows, which, use):
        for g in which:
            x = OX + 8 * g
            column = [u[c, b, OY + y + k - 1, x:x + 8, :] for k in range(rows + 2)]
            for k in range(rows):
                around = (column[k] + column[k + 2]) + (
                    u[c, b, OY + y + k, x - 1:x + 7, :] + u[c, b, OY + y + k, x + 1:x + 9, :])
                use(y + k, g, column[k + 1], f[c, y + k, 8 * g:8 * g + 8, :] + around)

    def regions(edge, middle):
        if edge:
            return ((0, 2, 1, every), (ny - 2, 2, 1, every), (2, 20, (ny - 4) // 20, rims))
        return ((2, 4, (ny - 4) // 4, inner),)

    def sweep(c, b, edge, final=False):
        def use(y, g, center, total):
            new = 0.2 * center + sol[y, 8 * g:8 * g + 8, lanes(c)] * total
            u[c, 1 - b, OY + y, OX + 8 * g:OX + 8 * g + 8, :] = new
            if final:
                sol[y, 8 * g:8 * g + 8, lanes(c)] = new
        for first, rows, count, which in regions(edge, not edge):
            over(first, rows, count, lambda y: stencil(c, b, y, rows, which, use))

    def defect(c, b, edge, use):
        def one(y, g, center, total):
            use(y, g, total - (4.0 + rem[y, 8 * g:8 * g + 8, lanes(c)]) * center)
        for first, rows, count, which in regions(edge, not edge):
            over(first, rows, count, lambda y: stencil(c, b, y, rows, which, one))

    def halve(row, col0, count, put):
        for g in range(count):
            at = 16 * (g + col0)
            even = spread[row, pl.ds(OX + at, 8, stride=2), :]
            odd = spread[row, pl.ds(OX + at + 1, 8, stride=2), :]
            put(g + col0, 0.5 * (even + odd))

    for c in range(chunks):
        fetched[3 * c].wait()

        def weigh(y):
            for g in every:
                pair = None
                for k in range(2):
                    mass = rem[y + k, 8 * g:8 * g + 8, lanes(c)]
                    sol[y + k, 8 * g:8 * g + 8, lanes(c)] = 0.8 / (4.0 + mass)
                    pair = mass if pair is None else pair + mass
                spread[y // 2 + 1, OX + 8 * g:OX + 8 * g + 8, :] = pair

        over(0, 2, my, weigh)

        def coarse_weight(j):
            def put(g, value):
                wide_weight[c, CY + j, CX + 8 * g:CX + 8 * g + 8, :] = 0.8 / (4.0 + value)
            halve(j + 1, 0, mx // 8, put)

        over(0, 1, my, coarse_weight)
        if c == 0:
            send_coarse(c, WEIGHT, wide_weight.at[c], FIRST)

    for c in range(chunks):
        fetched[3 * c + 1].wait()
        fetched[3 * c + 2].wait()
        arrive(c, U0)
        sweep(c, 0, True)
        send_fine(c, U1, 1)
        sweep(c, 0, False)
    for c in range(1, chunks):
        send_coarse(c, WEIGHT, wide_weight.at[c], FIRST)

    for c in range(chunks):
        arrive(c, U1)
        sweep(c, 1, True)
        send_fine(c, U2, 0)
        sweep(c, 1, False)

    for c in range(chunks):
        arrive(c, U2)
        for edge in (False, True):
            def keep(y, g, value):
                pass
            for first, rows, count, which in regions(edge, not edge):
                def part(y):
                    held = {}

                    def use(y_at, g, center, total):
                        value = total - (4.0 + rem[y_at, 8 * g:8 * g + 8, lanes(c)]) * center
                        if g in held:
                            row = held.pop(g)
                            spread[row[0], OX + 8 * g:OX + 8 * g + 8, :] = row[1] + value
                        else:
                            held[g] = (y_at // 2 + 1, value)
                    stencil(c, 0, y, rows, which, use)
                over(first, rows, count, part)

        def coarse_load(j):
            def put(g, value):
                wide_load[c, CY + j, CX + 8 * g:CX + 8 * g + 8, :] = value
            halve(j + 1, 0, mx // 8, put)

        over(0, 1, my, coarse_load)
        send_coarse(c, LOAD, wide_load.at[c], FIRST)

    own = tuple(range(CX, CX + mx, 8))

    def coarse_sweep(c, src, dst, depth):
        starts = (1,) + own + (CX + mx - 1,) if depth > 0 else own

        def row(y):
            for x in starts:
                around = (src[y - 1, x:x + 8, :] + src[y + 1, x:x + 8, :]) + (
                    src[y, x - 1:x + 7, :] + src[y, x + 1:x + 9, :])
                dst[y, x:x + 8, :] = 0.2 * src[y, x:x + 8, :] + wide_weight[c, y, x:x + 8, :] * (
                    wide_load[c, y, x:x + 8, :] + around)
        over(CY - depth, 2, (my + 2 * depth) // 2, lambda y: (row(y), row(y + 1)))

    for c in range(chunks):
        arrive(c, WEIGHT)
        arrive(c, LOAD)

        def first_sweep(y):
            for x in range(0, CX + mx + 8, 8):
                swap[0, y, x:x + 8, :] = wide_weight[c, y, x:x + 8, :] * wide_load[c, y, x:x + 8, :]
        over(CY - FIRST, 1, my + 2 * FIRST, first_sweep)
        at = 0
        for depth in range(FIRST - 1, 0, -1):
            coarse_sweep(c, swap.at[at], swap.at[1 - at], depth)
            at = 1 - at
        coarse_sweep(c, swap.at[at], wide_values.at[c], 0)
        send_coarse(c, COARSE, wide_values.at[c], SECOND)

    for c in range(chunks):
        arrive(c, COARSE)
        coarse_sweep(c, wide_values.at[c], swap.at[0], SECOND - 1)
        at = 0
        for depth in range(SECOND - 2, 0, -1):
            coarse_sweep(c, swap.at[at], swap.at[1 - at], depth)
            at = 1 - at

        def widen(j):
            for g in range((nx + 16) // 16):
                value = swap[at, CY - 1 + j, 4 + 8 * g:12 + 8 * g, :]
                spread[j, pl.ds(16 * g, 8, stride=2), :] = value
                spread[j, pl.ds(16 * g + 1, 8, stride=2), :] = value
        over(0, 1, my + 2, widen)

        def correct(y, j):
            for x in range(0, nx + 16, 8):
                u[c, 0, y, x:x + 8, :] = u[c, 0, y, x:x + 8, :] + spread[j, x:x + 8, :]
        correct(0, 0)
        over(0, 1, my, lambda j: (correct(2 * j + 1, j + 1), correct(2 * j + 2, j + 1)))
        correct(ny + 1, my + 1)
        sweep(c, 0, True)
        send_fine(c, U4, 1)
        sweep(c, 0, False)

    for c in range(chunks):
        arrive(c, U4)
        sweep(c, 1, True, final=True)
        send_fine(c, U5, 0)
        sweep(c, 1, False, final=True)

    for c in range(chunks):
        arrive(c, U5)

        def leave(y, g, value):
            rem[y, 8 * g:8 * g + 8, lanes(c)] = value
        defect(c, 0, False, leave)
        defect(c, 0, True, leave)


def local(source_terms, initial_values, absorption):
    ny, nx, layers = source_terms.shape
    chunks = layers // LANES
    wide = (ny // 2 + 2 * CY, nx // 2 + 2 * CX, LANES)
    rounds = 8
    return pl.pallas_call(
        functools.partial(kernel, (ny, nx, chunks)),
        out_shape=[pltpu.VMEM((ny, nx, layers), jnp.float32)] * 2,
        in_specs=[pl.BlockSpec(memory_space=pltpu.HBM)] * 3,
        out_specs=[pl.BlockSpec(memory_space=pltpu.VMEM)] * 2,
        scratch_shapes=[
            pltpu.VMEM((chunks, 2, ny + 2 * OY, nx + 2 * OX, LANES), jnp.float32),
            pltpu.VMEM((chunks, ny, nx, LANES), jnp.float32),
            pltpu.VMEM((chunks,) + wide, jnp.float32),
            pltpu.VMEM((chunks,) + wide, jnp.float32),
            pltpu.VMEM((chunks,) + wide, jnp.float32),
            pltpu.VMEM((2,) + wide, jnp.float32),
            pltpu.VMEM((ny // 2 + 2, nx + 2 * OX, LANES), jnp.float32),
            pltpu.SemaphoreType.DMA((3 * chunks,)),
            pltpu.SemaphoreType.DMA((chunks, rounds, len(AROUND))),
            pltpu.SemaphoreType.DMA((chunks, rounds, len(AROUND))),
        ],
        compiler_params=pltpu.CompilerParams(
            collective_id=0, has_side_effects=True, vmem_limit_bytes=46 * 1024 * 1024),
    )(source_terms, initial_values, absorption)


def solution(mesh):
    return jax.shard_map(
        local,
        mesh=mesh,
        in_specs=(P("py", "px", None),) * 3,
        out_specs=(P("py", "px", None),) * 2,
        check_vma=False,
    )
```

```python
import functools

import jax
import jax.numpy as jnp
from jax import lax
from jax.experimental import pallas as pl
from jax.experimental.pallas import tpu as pltpu
from jax.sharding import PartitionSpec as P

MESH = pl.DeviceIdType.MESH
LANES = 128
DEPTH = 3
GROUPS = 3
OY, OX = 1, 8
CY, CX = DEPTH, 8
SIDES = ((0, 1), (0, -1), (1, 0), (-1, 0))
CORNERS = ((1, 1), (1, -1), (-1, 1), (-1, -1))
AROUND = CORNERS + SIDES
U0, U1, U2, WEIGHT, LOAD, U4, U5, COARSE = range(8)
ROUNDS = COARSE + GROUPS - 1


def cut(direction, origin, size, depth, arriving):
    if direction == 0:
        return pl.ds(origin, size)
    if direction > 0:
        return pl.ds(origin - depth, depth) if arriving else pl.ds(origin + size - depth, depth)
    return pl.ds(origin + size, depth) if arriving else pl.ds(origin, depth)


def kernel(
    sizes, load_in, start_in, mass_in, sol, rem, u, f, wide, wide_values, swap, spread,
    local_sem, send_sem, recv_sem,
):
    ny, nx, chunks = sizes
    my, mx = ny // 2, nx // 2
    groups = nx // 8
    inner = tuple(range(1, groups - 1))
    rims = (0, groups - 1)
    every = tuple(range(groups))
    size_y, size_x = lax.axis_size("py"), lax.axis_size("px")
    at_y, at_x = lax.axis_index("py"), lax.axis_index("px")

    def device(dy, dx):
        return (lax.rem(at_y + dy + size_y, size_y), lax.rem(at_x + dx + size_x, size_x))

    def lanes(c):
        return pl.ds(c * LANES, LANES)

    def fetch(c, k):
        src, dst = (
            (start_in, u.at[c, 0, pl.ds(OY, ny), pl.ds(OX, nx), :]),
            (mass_in, rem.at[:, :, lanes(c)]),
            (load_in, f.at[c]),
        )[k]
        copy = pltpu.make_async_copy(src.at[:, :, lanes(c)], dst, local_sem.at[3 * c + k])
        copy.start()
        return copy

    started = [fetch(c, 0) for c in range(chunks)]
    weighed = [fetch(c, 1) for c in range(chunks)]
    loaded = [fetch(c, 2) for c in range(chunks)]

    barrier = pltpu.get_barrier_semaphore()
    for dy, dx in AROUND:
        pl.semaphore_signal(barrier, inc=1, device_id=device(dy, dx), device_id_type=MESH)
    pl.semaphore_wait(barrier, len(AROUND))

    flying = {}

    def send(c, tag, source, target, directions):
        copies = []
        for k, (dy, dx) in enumerate(directions):
            copy = pltpu.make_async_remote_copy(
                src_ref=source(dy, dx),
                dst_ref=target(dy, dx),
                send_sem=send_sem.at[c, tag, k],
                recv_sem=recv_sem.at[c, tag, k],
                device_id=device(dy, dx),
                device_id_type=MESH,
            )
            copy.start()
            copies.append(copy)
        flying[c, tag] = copies

    def arrive(c, tag):
        for copy in flying.pop((c, tag)):
            copy.wait()

    def fine_part(ref, dy, dx, arriving):
        return ref.at[cut(dy, OY, ny, 1, arriving), cut(dx, OX, nx, 1, arriving), :]

    def coarse_part(ref, dy, dx, arriving):
        depth = DEPTH - 1 if dy and dx else DEPTH
        return ref.at[cut(dy, CY, my, depth, arriving), cut(dx, CX, mx, depth, arriving), :]

    def send_fine(c, tag, b):
        send(c, tag, lambda dy, dx: fine_part(u.at[c, b], dy, dx, False),
             lambda dy, dx: fine_part(u.at[c, b], dy, dx, True), SIDES)

    def send_coarse(c, tag, ref, directions=AROUND, corners=None):
        def part(dy, dx, arriving):
            if dy and dx and corners is not None:
                depth = DEPTH - 1
                return corners.at[:, cut(dy, CY, my, depth, arriving), cut(dx, CX, mx, depth, arriving), :]
            return coarse_part(ref, dy, dx, arriving)
        send(c, tag, lambda dy, dx: part(dy, dx, False), lambda dy, dx: part(dy, dx, True), directions)

    for c in range(chunks):
        started[c].wait()
        send_fine(c, U0, 0)

    def over(first, rows, count, body):
        def step(i, carry):
            body(first + i * rows)
            return carry
        lax.fori_loop(0, count, step, 0)

    def stencil(c, b, y, rows, which, use):
        for g in which:
            x = OX + 8 * g
            column = [u[c, b, OY + y + k - 1, x:x + 8, :] for k in range(rows + 2)]
            for k in range(rows):
                around = (column[k] + column[k + 2]) + (
                    u[c, b, OY + y + k, x - 1:x + 7, :] + u[c, b, OY + y + k, x + 1:x + 9, :])
                use(y + k, g, column[k + 1], f[c, y + k, 8 * g:8 * g + 8, :] + around)

    def regions(edge, middle):
        if edge:
            return ((0, 2, 1, every), (ny - 2, 2, 1, every), (2, 20, (ny - 4) // 20, rims))
        return ((2, 4, (ny - 4) // 4, inner),)

    def sweep(c, b, edge, final=False):
        def use(y, g, center, total):
            new = 0.2 * center + sol[y, 8 * g:8 * g + 8, lanes(c)] * total
            u[c, 1 - b, OY + y, OX + 8 * g:OX + 8 * g + 8, :] = new
            if final:
                sol[y, 8 * g:8 * g + 8, lanes(c)] = new
        for first, rows, count, which in regions(edge, not edge):
            over(first, rows, count, lambda y: stencil(c, b, y, rows, which, use))

    def defect(c, b, edge, use):
        def one(y, g, center, total):
            use(y, g, total - (4.0 + rem[y, 8 * g:8 * g + 8, lanes(c)]) * center)
        for first, rows, count, which in regions(edge, not edge):
            over(first, rows, count, lambda y: stencil(c, b, y, rows, which, one))

    def halve(row, which, put):
        for g in which:
            even = spread[row, pl.ds(OX + 16 * g, 8, stride=2), :]
            odd = spread[row, pl.ds(OX + 16 * g + 1, 8, stride=2), :]
            put(g, 0.5 * (even + odd))

    for c in range(chunks):
        weighed[c].wait()

        def weigh(y):
            for g in every:
                pair = None
                for k in range(2):
                    mass = rem[y + k, 8 * g:8 * g + 8, lanes(c)]
                    sol[y + k, 8 * g:8 * g + 8, lanes(c)] = 0.8 / (4.0 + mass)
                    pair = mass if pair is None else pair + mass
                spread[y // 2 + 1, OX + 8 * g:OX + 8 * g + 8, :] = pair

        over(0, 2, my, weigh)

        def coarse_weight(j):
            def put(g, value):
                wide[c, 1, CY + j, CX + 8 * g:CX + 8 * g + 8, :] = 0.8 / (4.0 + value)
            halve(j + 1, range(mx // 8), put)

        over(0, 1, my, coarse_weight)
        if c == 0:
            send_coarse(c, WEIGHT, wide.at[c, 1], SIDES)

    for c in range(chunks):
        loaded[c].wait()
        arrive(c, U0)
        sweep(c, 0, True)
        send_fine(c, U1, 1)
        sweep(c, 0, False)
    for c in range(1, chunks):
        send_coarse(c, WEIGHT, wide.at[c, 1], SIDES)

    for c in range(chunks):
        arrive(c, U1)
        sweep(c, 1, True)
        send_fine(c, U2, 0)
        sweep(c, 1, False)

    for c in range(chunks):
        for edge in (False, True):
            if edge:
                arrive(c, U2)
            for first, rows, count, which in regions(edge, not edge):
                def part(y):
                    held = {}

                    def use(y_at, g, center, total):
                        value = total - (4.0 + rem[y_at, 8 * g:8 * g + 8, lanes(c)]) * center
                        if g in held:
                            row = held.pop(g)
                            spread[row[0], OX + 8 * g:OX + 8 * g + 8, :] = row[1] + value
                        else:
                            held[g] = (y_at // 2 + 1, value)
                    stencil(c, 0, y, rows, which, use)
                over(first, rows, count, part)

            def coarse_load(j, which):
                def put(g, value):
                    wide[c, 0, CY + j, CX + 8 * g:CX + 8 * g + 8, :] = value
                halve(j + 1, which, put)

            if edge:
                coarse_load(0, range(mx // 8))
                coarse_load(my - 1, range(mx // 8))
                over(1, 6, (my - 2) // 6, lambda j: [coarse_load(j + k, (0, mx // 8 - 1)) for k in range(6)])
            else:
                over(1, 2, (my - 2) // 2, lambda j: [coarse_load(j + k, range(1, mx // 8 - 1)) for k in range(2)])
        send_coarse(c, LOAD, wide.at[c, 0], corners=wide.at[c])

    own = tuple(range(CX, CX + mx, 8))

    def coarse_sweep(c, src, dst, depth):
        starts = (1,) + own + (CX + mx - 1,) if depth > 0 else own

        rows = 4 if (my + 2 * depth) % 4 == 0 else 2

        def some(y):
            for x in starts:
                column = [src[y + k - 1, x:x + 8, :] for k in range(rows + 2)]
                for k in range(rows):
                    around = (column[k] + column[k + 2]) + (
                        src[y + k, x - 1:x + 7, :] + src[y + k, x + 1:x + 9, :])
                    dst[y + k, x:x + 8, :] = 0.2 * column[k + 1] + wide[c, 1, y + k, x:x + 8, :] * (
                        wide[c, 0, y + k, x:x + 8, :] + around)
        over(CY - depth, rows, (my + 2 * depth) // rows, some)

    for c in range(chunks):
        arrive(c, WEIGHT)
        arrive(c, LOAD)

        def first_sweep(y):
            for k in range(2):
                for x in range(0, CX + mx + 8, 8):
                    swap[0, y + k, x:x + 8, :] = wide[c, 1, y + k, x:x + 8, :] * wide[c, 0, y + k, x:x + 8, :]
        over(CY - DEPTH, 2, (my + 2 * DEPTH) // 2, first_sweep)
        at = 0
        for depth in range(DEPTH - 1, 0, -1):
            coarse_sweep(c, swap.at[at], swap.at[1 - at], depth)
            at = 1 - at
        coarse_sweep(c, swap.at[at], wide_values.at[c, 0], 0)
        send_coarse(c, COARSE, wide_values.at[c, 0])

    for group in range(1, GROUPS - 1):
        for c in range(chunks):
            arrive(c, COARSE + group - 1)
            coarse_sweep(c, wide_values.at[c, group - 1], swap.at[0], DEPTH - 1)
            at = 0
            for depth in range(DEPTH - 2, 0, -1):
                coarse_sweep(c, swap.at[at], swap.at[1 - at], depth)
                at = 1 - at
            coarse_sweep(c, swap.at[at], wide_values.at[c, group], 0)
            send_coarse(c, COARSE + group, wide_values.at[c, group])

    for c in range(chunks):
        arrive(c, COARSE + GROUPS - 2)
        coarse_sweep(c, wide_values.at[c, GROUPS - 2], swap.at[0], DEPTH - 1)
        at = 0
        for depth in range(DEPTH - 2, 0, -1):
            coarse_sweep(c, swap.at[at], swap.at[1 - at], depth)
            at = 1 - at

        def widen(j):
            for g in range((nx + 16) // 16):
                value = swap[at, CY - 1 + j, 4 + 8 * g:12 + 8 * g, :]
                spread[j, pl.ds(16 * g, 8, stride=2), :] = value
                spread[j, pl.ds(16 * g + 1, 8, stride=2), :] = value
        over(0, 1, my + 2, widen)

        def correct(j, which):
            for x in which:
                for k in range(2):
                    u[c, 0, 2 * j - 1 + k, x:x + 8, :] = u[c, 0, 2 * j - 1 + k, x:x + 8, :] + spread[j, x:x + 8, :]

        across = tuple(range(0, nx + 16, 8))
        for y, j in ((0, 0), (ny + 1, my + 1)):
            for x in across:
                u[c, 0, y, x:x + 8, :] = u[c, 0, y, x:x + 8, :] + spread[j, x:x + 8, :]
        for j in (1, 2, my - 1, my):
            correct(j, across)
        over(3, 4, (my - 4) // 4, lambda j: [correct(j + k, across[:3] + across[-3:]) for k in range(4)])
        sweep(c, 0, True)
        send_fine(c, U4, 1)
        over(3, 2, (my - 4) // 2, lambda j: [correct(j + k, across[3:-3]) for k in range(2)])
        sweep(c, 0, False)

    for c in range(chunks):
        arrive(c, U4)
        sweep(c, 1, True, final=True)
        send_fine(c, U5, 0)
        sweep(c, 1, False, final=True)

    for c in range(chunks):
        def leave(y, g, value):
            rem[y, 8 * g:8 * g + 8, lanes(c)] = value
        defect(c, 0, False, leave)
        arrive(c, U5)
        defect(c, 0, True, leave)


def local(source_terms, initial_values, absorption):
    ny, nx, layers = source_terms.shape
    chunks = layers // LANES
    wide = (ny // 2 + 2 * CY, nx // 2 + 2 * CX, LANES)
    return pl.pallas_call(
        functools.partial(kernel, (ny, nx, chunks)),
        out_shape=[pltpu.VMEM((ny, nx, layers), jnp.float32)] * 2,
        in_specs=[pl.BlockSpec(memory_space=pltpu.HBM)] * 3,
        out_specs=[pl.BlockSpec(memory_space=pltpu.VMEM)] * 2,
        scratch_shapes=[
            pltpu.VMEM((chunks, 2, ny + 2 * OY, nx + 2 * OX, LANES), jnp.float32),
            pltpu.VMEM((chunks, ny, nx, LANES), jnp.float32),
            pltpu.VMEM((chunks, 2) + wide, jnp.float32),
            pltpu.VMEM((chunks, GROUPS - 1) + wide, jnp.float32),
            pltpu.VMEM((2,) + wide, jnp.float32),
            pltpu.VMEM((ny // 2 + 2, nx + 2 * OX, LANES), jnp.float32),
            pltpu.SemaphoreType.DMA((3 * chunks,)),
            pltpu.SemaphoreType.DMA((chunks, ROUNDS, len(AROUND))),
            pltpu.SemaphoreType.DMA((chunks, ROUNDS, len(AROUND))),
        ],
        compiler_params=pltpu.CompilerParams(
            collective_id=0, has_side_effects=True, vmem_limit_bytes=46 * 1024 * 1024),
    )(source_terms, initial_values, absorption)


def solution(mesh):
    return jax.shard_map(
        local,
        mesh=mesh,
        in_specs=(P("py", "px", None),) * 3,
        out_specs=(P("py", "px", None),) * 2,
        check_vma=False,
    )
```

```python
import functools

import jax
import jax.numpy as jnp
from jax import lax
from jax.experimental import pallas as pl
from jax.experimental.pallas import tpu as pltpu
from jax.sharding import PartitionSpec as P

MESH = pl.DeviceIdType.MESH
LANES = 128
DEPTH = 3
GROUPS = 3
OY, OX = 1, 8
CY, CX = DEPTH, 8
SIDES = ((0, 1), (0, -1), (1, 0), (-1, 0))
CORNERS = ((1, 1), (1, -1), (-1, 1), (-1, -1))
AROUND = CORNERS + SIDES
U0, U1, U2, WEIGHT, LINE, LOAD, U4, U5, COARSE = range(9)
ROUNDS = COARSE + GROUPS - 1


def cut(direction, origin, size, depth, arriving):
    if direction == 0:
        return pl.ds(origin, size)
    if direction > 0:
        return pl.ds(origin - depth, depth) if arriving else pl.ds(origin + size - depth, depth)
    return pl.ds(origin + size, depth) if arriving else pl.ds(origin, depth)


def kernel(
    sizes, load_in, start_in, mass_in, sol, rem, u, f, wide, wide_values, swap, spread,
    local_sem, send_sem, recv_sem,
):
    ny, nx, chunks = sizes
    my, mx = ny // 2, nx // 2
    groups = nx // 8
    inner = tuple(range(1, groups - 1))
    rims = (0, groups - 1)
    every = tuple(range(groups))
    size_y, size_x = lax.axis_size("py"), lax.axis_size("px")
    at_y, at_x = lax.axis_index("py"), lax.axis_index("px")

    def device(dy, dx):
        return (lax.rem(at_y + dy + size_y, size_y), lax.rem(at_x + dx + size_x, size_x))

    def lanes(c):
        return pl.ds(c * LANES, LANES)

    def fetch(c, k):
        src, dst = (
            (start_in, u.at[c, 0, pl.ds(OY, ny), pl.ds(OX, nx), :]),
            (mass_in, rem.at[:, :, lanes(c)]),
            (load_in, f.at[c]),
        )[k]
        copy = pltpu.make_async_copy(src.at[:, :, lanes(c)], dst, local_sem.at[3 * c + k])
        copy.start()
        return copy

    started = [fetch(c, 0) for c in range(chunks)]
    weighed = [fetch(c, 1) for c in range(chunks)]
    loaded = [fetch(c, 2) for c in range(chunks)]

    one = jnp.ones((8, LANES), jnp.float32)
    for c in range(chunks):
        for x in range(CX, CX + mx, 8):
            wide[c, 1, CY - DEPTH, x:x + 8, :] = one
            wide[c, 1, CY + my + DEPTH - 1, x:x + 8, :] = one

        def sides(i, carry):
            wide[c, 1, CY + i, 0:8, :] = one
            wide[c, 1, CY + i, CX + mx:CX + mx + 8, :] = one
            return carry
        lax.fori_loop(0, my, sides, 0)

    barrier = pltpu.get_barrier_semaphore()
    for dy, dx in AROUND:
        pl.semaphore_signal(barrier, inc=1, device_id=device(dy, dx), device_id_type=MESH)
    pl.semaphore_wait(barrier, len(AROUND))

    flying = {}

    def send(c, tag, source, target, directions):
        copies = []
        for k, (dy, dx) in enumerate(directions):
            copy = pltpu.make_async_remote_copy(
                src_ref=source(dy, dx),
                dst_ref=target(dy, dx),
                send_sem=send_sem.at[c, tag, k],
                recv_sem=recv_sem.at[c, tag, k],
                device_id=device(dy, dx),
                device_id_type=MESH,
            )
            copy.start()
            copies.append(copy)
        flying[c, tag] = copies

    def arrive(c, tag):
        for copy in flying.pop((c, tag)):
            copy.wait()

    def fine_part(ref, dy, dx, arriving):
        return ref.at[cut(dy, OY, ny, 1, arriving), cut(dx, OX, nx, 1, arriving), :]

    def coarse_part(ref, dy, dx, arriving, depth=DEPTH):
        depth = DEPTH - 1 if dy and dx else depth
        return ref.at[cut(dy, CY, my, depth, arriving), cut(dx, CX, mx, depth, arriving), :]

    def send_fine(c, tag, b):
        send(c, tag, lambda dy, dx: fine_part(u.at[c, b], dy, dx, False),
             lambda dy, dx: fine_part(u.at[c, b], dy, dx, True), SIDES)

    def send_coarse(c, tag, ref, directions=AROUND, corners=None, sides=DEPTH):
        def part(dy, dx, arriving):
            if dy and dx and corners is not None:
                depth = DEPTH - 1
                return corners.at[:, cut(dy, CY, my, depth, arriving), cut(dx, CX, mx, depth, arriving), :]
            return coarse_part(ref, dy, dx, arriving, sides)
        send(c, tag, lambda dy, dx: part(dy, dx, False), lambda dy, dx: part(dy, dx, True), directions)

    def line(direction, origin, size, arriving):
        if direction == 0:
            return pl.ds(origin, size)
        if direction > 0:
            return pl.ds(origin - DEPTH if arriving else origin + size - DEPTH, 1)
        return pl.ds(origin + size + DEPTH - 1 if arriving else origin + DEPTH - 1, 1)

    def send_line(c):
        def part(ref, dy, dx, arriving):
            return ref.at[line(dy, CY, my, arriving), line(dx, CX, mx, arriving), :]
        send(c, LINE, lambda dy, dx: part(wide_values.at[c, 1], dy, dx, False),
             lambda dy, dx: part(wide.at[c, 0], dy, dx, True), SIDES)

    for c in range(chunks):
        started[c].wait()
        send_fine(c, U0, 0)

    def over(first, rows, count, body):
        def step(i, carry):
            body(first + i * rows)
            return carry
        lax.fori_loop(0, count, step, 0)

    def stencil(c, b, y, rows, which, use):
        for g in which:
            x = OX + 8 * g
            column = [u[c, b, OY + y + k - 1, x:x + 8, :] for k in range(rows + 2)]
            for k in range(rows):
                around = (column[k] + column[k + 2]) + (
                    u[c, b, OY + y + k, x - 1:x + 7, :] + u[c, b, OY + y + k, x + 1:x + 9, :])
                use(y + k, g, column[k + 1], f[c, y + k, 8 * g:8 * g + 8, :] + around)

    def regions(edge, middle):
        if edge:
            return ((0, 2, 1, every), (ny - 2, 2, 1, every), (2, 20, (ny - 4) // 20, rims))
        return ((2, 4, (ny - 4) // 4, inner),)

    def sweep(c, b, edge, final=False):
        def use(y, g, center, total):
            new = 0.2 * center + sol[y, 8 * g:8 * g + 8, lanes(c)] * total
            u[c, 1 - b, OY + y, OX + 8 * g:OX + 8 * g + 8, :] = new
            if final:
                sol[y, 8 * g:8 * g + 8, lanes(c)] = new
        for first, rows, count, which in regions(edge, not edge):
            over(first, rows, count, lambda y: stencil(c, b, y, rows, which, use))

    def defect(c, b, edge, use):
        def one(y, g, center, total):
            use(y, g, total - (4.0 + rem[y, 8 * g:8 * g + 8, lanes(c)]) * center)
        for first, rows, count, which in regions(edge, not edge):
            over(first, rows, count, lambda y: stencil(c, b, y, rows, which, one))

    def halve(row, which, put):
        for g in which:
            even = spread[row, pl.ds(OX + 16 * g, 8, stride=2), :]
            odd = spread[row, pl.ds(OX + 16 * g + 1, 8, stride=2), :]
            put(g, 0.5 * (even + odd))

    for c in range(chunks):
        weighed[c].wait()

        def weigh(y):
            for g in every:
                pair = None
                for k in range(2):
                    mass = rem[y + k, 8 * g:8 * g + 8, lanes(c)]
                    sol[y + k, 8 * g:8 * g + 8, lanes(c)] = 0.8 / (4.0 + mass)
                    pair = mass if pair is None else pair + mass
                spread[y // 2 + 1, OX + 8 * g:OX + 8 * g + 8, :] = pair

        over(0, 2, my, weigh)

        def coarse_weight(j):
            def put(g, value):
                wide[c, 1, CY + j, CX + 8 * g:CX + 8 * g + 8, :] = 0.8 / (4.0 + value)
            halve(j + 1, range(mx // 8), put)

        over(0, 1, my, coarse_weight)
        if c == 0:
            send_coarse(c, WEIGHT, wide.at[c, 1], SIDES, sides=DEPTH - 1)

    for c in range(chunks):
        loaded[c].wait()
        arrive(c, U0)
        sweep(c, 0, True)
        send_fine(c, U1, 1)
        sweep(c, 0, False)
    for c in range(1, chunks):
        send_coarse(c, WEIGHT, wide.at[c, 1], SIDES, sides=DEPTH - 1)

    for c in range(chunks):
        arrive(c, U1)
        sweep(c, 1, True)
        send_fine(c, U2, 0)
        sweep(c, 1, False)

    for c in range(chunks):
        for edge in (False, True):
            if edge:
                arrive(c, U2)
            for first, rows, count, which in regions(edge, not edge):
                def part(y):
                    held = {}

                    def use(y_at, g, center, total):
                        value = total - (4.0 + rem[y_at, 8 * g:8 * g + 8, lanes(c)]) * center
                        if g in held:
                            row = held.pop(g)
                            spread[row[0], OX + 8 * g:OX + 8 * g + 8, :] = row[1] + value
                        else:
                            held[g] = (y_at // 2 + 1, value)
                    stencil(c, 0, y, rows, which, use)
                over(first, rows, count, part)

            def coarse_load(j, which):
                def put(g, value):
                    here = (CY + j, slice(CX + 8 * g, CX + 8 * g + 8))
                    wide[(c, 0) + here] = value
                    wide_values[(c, 1) + here] = wide[(c, 1) + here] * value
                halve(j + 1, which, put)

            if edge:
                coarse_load(0, range(mx // 8))
                coarse_load(my - 1, range(mx // 8))
                over(1, 6, (my - 2) // 6, lambda j: [coarse_load(j + k, (0, mx // 8 - 1)) for k in range(6)])
            else:
                over(1, 2, (my - 2) // 2, lambda j: [coarse_load(j + k, range(1, mx // 8 - 1)) for k in range(2)])
        send_line(c)
        send_coarse(c, LOAD, wide.at[c, 0], corners=wide.at[c], sides=DEPTH - 1)

    own = tuple(range(CX, CX + mx, 8))

    def coarse_sweep(c, src, dst, depth):
        starts = (1,) + own + (CX + mx - 1,) if depth > 0 else own

        rows = 4 if (my + 2 * depth) % 4 == 0 else 2

        def some(y):
            for x in starts:
                column = [src[y + k - 1, x:x + 8, :] for k in range(rows + 2)]
                for k in range(rows):
                    around = (column[k] + column[k + 2]) + (
                        src[y + k, x - 1:x + 7, :] + src[y + k, x + 1:x + 9, :])
                    dst[y + k, x:x + 8, :] = 0.2 * column[k + 1] + wide[c, 1, y + k, x:x + 8, :] * (
                        wide[c, 0, y + k, x:x + 8, :] + around)
        over(CY - depth, rows, (my + 2 * depth) // rows, some)

    for c in range(chunks):
        arrive(c, WEIGHT)
        arrive(c, LINE)
        arrive(c, LOAD)

        def first_sweep(y):
            for k in range(2):
                for x in range(0, CX + mx + 8, 8):
                    swap[0, y + k, x:x + 8, :] = wide[c, 1, y + k, x:x + 8, :] * wide[c, 0, y + k, x:x + 8, :]
        over(CY - DEPTH, 2, (my + 2 * DEPTH) // 2, first_sweep)
        at = 0
        for depth in range(DEPTH - 1, 0, -1):
            coarse_sweep(c, swap.at[at], swap.at[1 - at], depth)
            at = 1 - at
        coarse_sweep(c, swap.at[at], wide_values.at[c, 0], 0)
        send_coarse(c, COARSE, wide_values.at[c, 0])

    for group in range(1, GROUPS - 1):
        for c in range(chunks):
            arrive(c, COARSE + group - 1)
            coarse_sweep(c, wide_values.at[c, group - 1], swap.at[0], DEPTH - 1)
            at = 0
            for depth in range(DEPTH - 2, 0, -1):
                coarse_sweep(c, swap.at[at], swap.at[1 - at], depth)
                at = 1 - at
            coarse_sweep(c, swap.at[at], wide_values.at[c, group], 0)
            send_coarse(c, COARSE + group, wide_values.at[c, group])

    for c in range(chunks):
        arrive(c, COARSE + GROUPS - 2)
        coarse_sweep(c, wide_values.at[c, GROUPS - 2], swap.at[0], DEPTH - 1)
        at = 0
        for depth in range(DEPTH - 2, 0, -1):
            coarse_sweep(c, swap.at[at], swap.at[1 - at], depth)
            at = 1 - at

        def widen(j):
            for g in range((nx + 16) // 16):
                value = swap[at, CY - 1 + j, 4 + 8 * g:12 + 8 * g, :]
                spread[j, pl.ds(16 * g, 8, stride=2), :] = value
                spread[j, pl.ds(16 * g + 1, 8, stride=2), :] = value
        over(0, 1, my + 2, widen)

        def correct(j, which):
            for x in which:
                for k in range(2):
                    u[c, 0, 2 * j - 1 + k, x:x + 8, :] = u[c, 0, 2 * j - 1 + k, x:x + 8, :] + spread[j, x:x + 8, :]

        across = tuple(range(0, nx + 16, 8))
        for y, j in ((0, 0), (ny + 1, my + 1)):
            for x in across:
                u[c, 0, y, x:x + 8, :] = u[c, 0, y, x:x + 8, :] + spread[j, x:x + 8, :]
        for j in (1, 2, my - 1, my):
            correct(j, across)
        over(3, 4, (my - 4) // 4, lambda j: [correct(j + k, across[:3] + across[-3:]) for k in range(4)])
        sweep(c, 0, True)
        send_fine(c, U4, 1)
        over(3, 2, (my - 4) // 2, lambda j: [correct(j + k, across[3:-3]) for k in range(2)])
        sweep(c, 0, False)

    for c in range(chunks):
        arrive(c, U4)
        sweep(c, 1, True, final=True)
        send_fine(c, U5, 0)
        sweep(c, 1, False, final=True)

    for c in range(chunks):
        def leave(y, g, value):
            rem[y, 8 * g:8 * g + 8, lanes(c)] = value
        defect(c, 0, False, leave)
        arrive(c, U5)
        defect(c, 0, True, leave)


PIECES = 4


def deliver(sol, rem, sol_out, rem_out, sems):
    rows = sol.shape[0] // PIECES
    copies = []
    for k in range(PIECES):
        for n, (src, dst) in enumerate(((sol, sol_out), (rem, rem_out))):
            part = pl.ds(k * rows, rows)
            copies.append(pltpu.make_async_copy(src.at[part], dst.at[part], sems.at[n, k]))
    for copy in copies:
        copy.start()
    for copy in copies:
        copy.wait()


def local(source_terms, initial_values, absorption):
    ny, nx, layers = source_terms.shape
    chunks = layers // LANES
    wide = (ny // 2 + 2 * CY, nx // 2 + 2 * CX, LANES)
    held = pl.pallas_call(
        functools.partial(kernel, (ny, nx, chunks)),
        out_shape=[pltpu.VMEM((ny, nx, layers), jnp.float32)] * 2,
        in_specs=[pl.BlockSpec(memory_space=pltpu.HBM)] * 3,
        out_specs=[pl.BlockSpec(memory_space=pltpu.VMEM)] * 2,
        scratch_shapes=[
            pltpu.VMEM((chunks, 2, ny + 2 * OY, nx + 2 * OX, LANES), jnp.float32),
            pltpu.VMEM((chunks, ny, nx, LANES), jnp.float32),
            pltpu.VMEM((chunks, 2) + wide, jnp.float32),
            pltpu.VMEM((chunks, GROUPS - 1) + wide, jnp.float32),
            pltpu.VMEM((2,) + wide, jnp.float32),
            pltpu.VMEM((ny // 2 + 2, nx + 2 * OX, LANES), jnp.float32),
            pltpu.SemaphoreType.DMA((3 * chunks,)),
            pltpu.SemaphoreType.DMA((chunks, ROUNDS, len(AROUND))),
            pltpu.SemaphoreType.DMA((chunks, ROUNDS, len(AROUND))),
        ],
        compiler_params=pltpu.CompilerParams(
            collective_id=0, has_side_effects=True, vmem_limit_bytes=46 * 1024 * 1024),
    )(source_terms, initial_values, absorption)
    return pl.pallas_call(
        deliver,
        out_shape=[jax.ShapeDtypeStruct((ny, nx, layers), jnp.float32)] * 2,
        in_specs=[pl.BlockSpec(memory_space=pltpu.VMEM)] * 2,
        out_specs=[pl.BlockSpec(memory_space=pltpu.HBM)] * 2,
        scratch_shapes=[pltpu.SemaphoreType.DMA((2, PIECES))],
        compiler_params=pltpu.CompilerParams(vmem_limit_bytes=20 * 1024 * 1024),
    )(*held)


def solution(mesh):
    return jax.shard_map(
        local,
        mesh=mesh,
        in_specs=(P("py", "px", None),) * 3,
        out_specs=(P("py", "px", None),) * 2,
        check_vma=False,
    )
```

```python
import functools

import jax
import jax.numpy as jnp
from jax import lax
from jax.experimental import pallas as pl
from jax.experimental.pallas import tpu as pltpu
from jax.sharding import PartitionSpec as P

MESH = pl.DeviceIdType.MESH
LANES = 128
DEPTH = 3
GROUPS = 3
OY, OX = 1, 8
CY, CX = DEPTH, 8
SIDES = ((0, 1), (0, -1), (1, 0), (-1, 0))
CORNERS = ((1, 1), (1, -1), (-1, 1), (-1, -1))
AROUND = CORNERS + SIDES
U0, U1, U2, WEIGHT, LINE, LOAD, U4, U5, LAST, COARSE = range(10)
ROUNDS = COARSE + GROUPS - 1


def cut(direction, origin, size, depth, arriving):
    if direction == 0:
        return pl.ds(origin, size)
    if direction > 0:
        return pl.ds(origin - depth, depth) if arriving else pl.ds(origin + size - depth, depth)
    return pl.ds(origin + size, depth) if arriving else pl.ds(origin, depth)


def kernel(
    sizes, load_in, start_in, mass_in, sol, rem, u, f, wide, wide_values, swap, spread,
    local_sem, send_sem, recv_sem,
):
    ny, nx, chunks = sizes
    my, mx = ny // 2, nx // 2
    groups = nx // 8
    inner = tuple(range(1, groups - 1))
    rims = (0, groups - 1)
    every = tuple(range(groups))
    size_y, size_x = lax.axis_size("py"), lax.axis_size("px")
    at_y, at_x = lax.axis_index("py"), lax.axis_index("px")

    def device(dy, dx):
        return (lax.rem(at_y + dy + size_y, size_y), lax.rem(at_x + dx + size_x, size_x))

    def lanes(c):
        return pl.ds(c * LANES, LANES)

    def fetch(c, k):
        src, dst = (
            (start_in, u.at[c, 0, pl.ds(OY, ny), pl.ds(OX, nx), :]),
            (mass_in, rem.at[:, :, lanes(c)]),
            (load_in, f.at[c]),
        )[k]
        copy = pltpu.make_async_copy(src.at[:, :, lanes(c)], dst, local_sem.at[3 * c + k])
        copy.start()
        return copy

    started = [fetch(c, 0) for c in range(chunks)]
    weighed = [fetch(c, 1) for c in range(chunks)]
    loaded = [fetch(c, 2) for c in range(chunks)]

    one = jnp.ones((8, LANES), jnp.float32)
    for c in range(chunks):
        for x in range(CX, CX + mx, 8):
            wide[c, 1, CY - DEPTH, x:x + 8, :] = one
            wide[c, 1, CY + my + DEPTH - 1, x:x + 8, :] = one

        def sides(i, carry):
            wide[c, 1, CY + i, 0:8, :] = one
            wide[c, 1, CY + i, CX + mx:CX + mx + 8, :] = one
            return carry
        lax.fori_loop(0, my, sides, 0)

    barrier = pltpu.get_barrier_semaphore()
    for dy, dx in AROUND:
        pl.semaphore_signal(barrier, inc=1, device_id=device(dy, dx), device_id_type=MESH)
    pl.semaphore_wait(barrier, len(AROUND))

    flying = {}

    def send(c, tag, source, target, directions):
        copies = []
        for k, (dy, dx) in enumerate(directions):
            copy = pltpu.make_async_remote_copy(
                src_ref=source(dy, dx),
                dst_ref=target(dy, dx),
                send_sem=send_sem.at[c, tag, k],
                recv_sem=recv_sem.at[c, tag, k],
                device_id=device(dy, dx),
                device_id_type=MESH,
            )
            copy.start()
            copies.append(copy)
        flying[c, tag] = copies

    def arrive(c, tag):
        for copy in flying.pop((c, tag)):
            copy.wait()

    def fine_part(ref, dy, dx, arriving):
        return ref.at[cut(dy, OY, ny, 1, arriving), cut(dx, OX, nx, 1, arriving), :]

    def coarse_part(ref, dy, dx, arriving, depth=DEPTH):
        depth = DEPTH - 1 if dy and dx else depth
        return ref.at[cut(dy, CY, my, depth, arriving), cut(dx, CX, mx, depth, arriving), :]

    def send_fine(c, tag, b):
        send(c, tag, lambda dy, dx: fine_part(u.at[c, b], dy, dx, False),
             lambda dy, dx: fine_part(u.at[c, b], dy, dx, True), SIDES)

    def send_coarse(c, tag, ref, directions=AROUND, corners=None, sides=DEPTH):
        def part(dy, dx, arriving):
            if dy and dx and corners is not None:
                depth = DEPTH - 1
                return corners.at[:, cut(dy, CY, my, depth, arriving), cut(dx, CX, mx, depth, arriving), :]
            return coarse_part(ref, dy, dx, arriving, sides)
        send(c, tag, lambda dy, dx: part(dy, dx, False), lambda dy, dx: part(dy, dx, True), directions)

    def line(direction, origin, size, arriving):
        if direction == 0:
            return pl.ds(origin, size)
        if direction > 0:
            return pl.ds(origin - DEPTH if arriving else origin + size - DEPTH, 1)
        return pl.ds(origin + size + DEPTH - 1 if arriving else origin + DEPTH - 1, 1)

    def send_line(c, tag, directions):
        def part(ref, dy, dx, arriving):
            return ref.at[line(dy, CY, my, arriving), line(dx, CX, mx, arriving), :]
        send(c, tag, lambda dy, dx: part(wide_values.at[c, 1], dy, dx, False),
             lambda dy, dx: part(wide.at[c, 0], dy, dx, True), directions)

    for c in range(chunks):
        started[c].wait()
        send_fine(c, U0, 0)

    def over(first, rows, count, body):
        def step(i, carry):
            body(first + i * rows)
            return carry
        lax.fori_loop(0, count, step, 0)

    def stencil(c, b, y, rows, which, use):
        for g in which:
            x = OX + 8 * g
            column = [u[c, b, OY + y + k - 1, x:x + 8, :] for k in range(rows + 2)]
            for k in range(rows):
                around = (column[k] + column[k + 2]) + (
                    u[c, b, OY + y + k, x - 1:x + 7, :] + u[c, b, OY + y + k, x + 1:x + 9, :])
                use(y + k, g, column[k + 1], f[c, y + k, 8 * g:8 * g + 8, :] + around)

    def regions(edge, middle):
        if edge:
            return ((0, 2, 1, every), (ny - 2, 2, 1, every), (2, 20, (ny - 4) // 20, rims))
        return ((2, 4, (ny - 4) // 4, inner),)

    def sweep(c, b, edge, final=False):
        def use(y, g, center, total):
            new = 0.2 * center + sol[y, 8 * g:8 * g + 8, lanes(c)] * total
            u[c, 1 - b, OY + y, OX + 8 * g:OX + 8 * g + 8, :] = new
            if final:
                sol[y, 8 * g:8 * g + 8, lanes(c)] = new
        for first, rows, count, which in regions(edge, not edge):
            over(first, rows, count, lambda y: stencil(c, b, y, rows, which, use))

    def defect(c, b, edge, use):
        def one(y, g, center, total):
            use(y, g, total - (4.0 + rem[y, 8 * g:8 * g + 8, lanes(c)]) * center)
        for first, rows, count, which in regions(edge, not edge):
            over(first, rows, count, lambda y: stencil(c, b, y, rows, which, one))

    def halve(row, which, put):
        for g in which:
            even = spread[row, pl.ds(OX + 16 * g, 8, stride=2), :]
            odd = spread[row, pl.ds(OX + 16 * g + 1, 8, stride=2), :]
            put(g, 0.5 * (even + odd))

    for c in range(chunks):
        weighed[c].wait()

        def weigh(y):
            for g in every:
                pair = None
                for k in range(2):
                    mass = rem[y + k, 8 * g:8 * g + 8, lanes(c)]
                    sol[y + k, 8 * g:8 * g + 8, lanes(c)] = 0.8 / (4.0 + mass)
                    pair = mass if pair is None else pair + mass
                spread[y // 2 + 1, OX + 8 * g:OX + 8 * g + 8, :] = pair

        over(0, 2, my, weigh)

        def coarse_weight(j):
            def put(g, value):
                wide[c, 1, CY + j, CX + 8 * g:CX + 8 * g + 8, :] = 0.8 / (4.0 + value)
            halve(j + 1, range(mx // 8), put)

        over(0, 1, my, coarse_weight)
        if c == 0:
            send_coarse(c, WEIGHT, wide.at[c, 1], SIDES, sides=DEPTH - 1)

    for c in range(chunks):
        loaded[c].wait()
        arrive(c, U0)
        sweep(c, 0, True)
        send_fine(c, U1, 1)
        sweep(c, 0, False)
    for c in range(1, chunks):
        send_coarse(c, WEIGHT, wide.at[c, 1], SIDES, sides=DEPTH - 1)

    for c in range(chunks):
        arrive(c, U1)
        sweep(c, 1, True)
        send_fine(c, U2, 0)
        sweep(c, 1, False)

    for c in range(chunks):
        for edge in (False, True):
            if edge:
                arrive(c, U2)
            for first, rows, count, which in regions(edge, not edge):
                def part(y):
                    held = {}

                    def use(y_at, g, center, total):
                        value = total - (4.0 + rem[y_at, 8 * g:8 * g + 8, lanes(c)]) * center
                        if g in held:
                            row = held.pop(g)
                            spread[row[0], OX + 8 * g:OX + 8 * g + 8, :] = row[1] + value
                        else:
                            held[g] = (y_at // 2 + 1, value)
                    stencil(c, 0, y, rows, which, use)
                over(first, rows, count, part)

            def coarse_load(j, which):
                def put(g, value):
                    here = (CY + j, slice(CX + 8 * g, CX + 8 * g + 8))
                    wide[(c, 0) + here] = value
                    wide_values[(c, 1) + here] = wide[(c, 1) + here] * value
                halve(j + 1, which, put)

            if edge:
                coarse_load(0, range(mx // 8))
                coarse_load(my - 1, range(mx // 8))
                over(1, 6, (my - 2) // 6, lambda j: [coarse_load(j + k, (0, mx // 8 - 1)) for k in range(6)])
            else:
                over(1, 2, (my - 2) // 2, lambda j: [coarse_load(j + k, range(1, mx // 8 - 1)) for k in range(2)])
        send_line(c, LINE, SIDES[:2])
        send_coarse(c, LOAD, wide.at[c, 0], corners=wide.at[c], sides=DEPTH - 1)
        send_line(c, LAST, SIDES[2:])

    own = tuple(range(CX, CX + mx, 8))

    def coarse_sweep(c, src, dst, depth):
        starts = (1,) + own + (CX + mx - 1,) if depth > 0 else own

        rows = 4 if (my + 2 * depth) % 4 == 0 else 2

        def some(y):
            for x in starts:
                column = [src[y + k - 1, x:x + 8, :] for k in range(rows + 2)]
                for k in range(rows):
                    around = (column[k] + column[k + 2]) + (
                        src[y + k, x - 1:x + 7, :] + src[y + k, x + 1:x + 9, :])
                    dst[y + k, x:x + 8, :] = 0.2 * column[k + 1] + wide[c, 1, y + k, x:x + 8, :] * (
                        wide[c, 0, y + k, x:x + 8, :] + around)
        over(CY - depth, rows, (my + 2 * depth) // rows, some)

    for c in range(chunks):
        arrive(c, WEIGHT)
        arrive(c, LINE)
        arrive(c, LOAD)
        arrive(c, LAST)

        def first_sweep(y):
            for k in range(2):
                for x in range(0, CX + mx + 8, 8):
                    swap[0, y + k, x:x + 8, :] = wide[c, 1, y + k, x:x + 8, :] * wide[c, 0, y + k, x:x + 8, :]
        over(CY - DEPTH, 2, (my + 2 * DEPTH) // 2, first_sweep)
        at = 0
        for depth in range(DEPTH - 1, 0, -1):
            coarse_sweep(c, swap.at[at], swap.at[1 - at], depth)
            at = 1 - at
        coarse_sweep(c, swap.at[at], wide_values.at[c, 0], 0)
        send_coarse(c, COARSE, wide_values.at[c, 0])

    for group in range(1, GROUPS - 1):
        for c in range(chunks):
            arrive(c, COARSE + group - 1)
            coarse_sweep(c, wide_values.at[c, group - 1], swap.at[0], DEPTH - 1)
            at = 0
            for depth in range(DEPTH - 2, 0, -1):
                coarse_sweep(c, swap.at[at], swap.at[1 - at], depth)
                at = 1 - at
            coarse_sweep(c, swap.at[at], wide_values.at[c, group], 0)
            send_coarse(c, COARSE + group, wide_values.at[c, group])

    for c in range(chunks):
        arrive(c, COARSE + GROUPS - 2)
        coarse_sweep(c, wide_values.at[c, GROUPS - 2], swap.at[0], DEPTH - 1)
        at = 0
        for depth in range(DEPTH - 2, 0, -1):
            coarse_sweep(c, swap.at[at], swap.at[1 - at], depth)
            at = 1 - at

        def widen(j):
            for g in range((nx + 16) // 16):
                value = swap[at, CY - 1 + j, 4 + 8 * g:12 + 8 * g, :]
                spread[j, pl.ds(16 * g, 8, stride=2), :] = value
                spread[j, pl.ds(16 * g + 1, 8, stride=2), :] = value
        over(0, 1, my + 2, widen)

        def correct(j, which):
            for x in which:
                for k in range(2):
                    u[c, 0, 2 * j - 1 + k, x:x + 8, :] = u[c, 0, 2 * j - 1 + k, x:x + 8, :] + spread[j, x:x + 8, :]

        across = tuple(range(0, nx + 16, 8))
        for y, j in ((0, 0), (ny + 1, my + 1)):
            for x in across:
                u[c, 0, y, x:x + 8, :] = u[c, 0, y, x:x + 8, :] + spread[j, x:x + 8, :]
        for j in (1, 2, my - 1, my):
            correct(j, across)
        over(3, 4, (my - 4) // 4, lambda j: [correct(j + k, across[:3] + across[-3:]) for k in range(4)])
        sweep(c, 0, True)
        send_fine(c, U4, 1)
        over(3, 2, (my - 4) // 2, lambda j: [correct(j + k, across[3:-3]) for k in range(2)])
        sweep(c, 0, False)

    for c in range(chunks):
        arrive(c, U4)
        sweep(c, 1, True, final=True)
        send_fine(c, U5, 0)
        sweep(c, 1, False, final=True)

    for c in range(chunks):
        def leave(y, g, value):
            rem[y, 8 * g:8 * g + 8, lanes(c)] = value
        defect(c, 0, False, leave)
        arrive(c, U5)
        defect(c, 0, True, leave)


PIECES = 4


def deliver(sol, rem, sol_out, rem_out, sems):
    rows = sol.shape[0] // PIECES
    copies = []
    for k in range(PIECES):
        for n, (src, dst) in enumerate(((sol, sol_out), (rem, rem_out))):
            part = pl.ds(k * rows, rows)
            copies.append(pltpu.make_async_copy(src.at[part], dst.at[part], sems.at[n, k]))
    for copy in copies:
        copy.start()
    for copy in copies:
        copy.wait()


def local(source_terms, initial_values, absorption):
    ny, nx, layers = source_terms.shape
    chunks = layers // LANES
    wide = (ny // 2 + 2 * CY, nx // 2 + 2 * CX, LANES)
    held = pl.pallas_call(
        functools.partial(kernel, (ny, nx, chunks)),
        out_shape=[pltpu.VMEM((ny, nx, layers), jnp.float32)] * 2,
        in_specs=[pl.BlockSpec(memory_space=pltpu.HBM)] * 3,
        out_specs=[pl.BlockSpec(memory_space=pltpu.VMEM)] * 2,
        scratch_shapes=[
            pltpu.VMEM((chunks, 2, ny + 2 * OY, nx + 2 * OX, LANES), jnp.float32),
            pltpu.VMEM((chunks, ny, nx, LANES), jnp.float32),
            pltpu.VMEM((chunks, 2) + wide, jnp.float32),
            pltpu.VMEM((chunks, GROUPS - 1) + wide, jnp.float32),
            pltpu.VMEM((2,) + wide, jnp.float32),
            pltpu.VMEM((ny // 2 + 2, nx + 2 * OX, LANES), jnp.float32),
            pltpu.SemaphoreType.DMA((3 * chunks,)),
            pltpu.SemaphoreType.DMA((chunks, ROUNDS, len(AROUND))),
            pltpu.SemaphoreType.DMA((chunks, ROUNDS, len(AROUND))),
        ],
        compiler_params=pltpu.CompilerParams(
            collective_id=0, has_side_effects=True, vmem_limit_bytes=46 * 1024 * 1024),
    )(source_terms, initial_values, absorption)
    return pl.pallas_call(
        deliver,
        out_shape=[jax.ShapeDtypeStruct((ny, nx, layers), jnp.float32)] * 2,
        in_specs=[pl.BlockSpec(memory_space=pltpu.VMEM)] * 2,
        out_specs=[pl.BlockSpec(memory_space=pltpu.HBM)] * 2,
        scratch_shapes=[pltpu.SemaphoreType.DMA((2, PIECES))],
        compiler_params=pltpu.CompilerParams(vmem_limit_bytes=20 * 1024 * 1024),
    )(*held)


def solution(mesh):
    return jax.shard_map(
        local,
        mesh=mesh,
        in_specs=(P("py", "px", None),) * 3,
        out_specs=(P("py", "px", None),) * 2,
        check_vma=False,
    )
```
